32 devices in a mesh: seq: 8 (over z, x), head: 4 (over y, core).
Axes of the slice: x: 2, y: 2, z: 4, core: 2. Of those that a mesh axis runs over, the one named last changes fastest.
Arguments:
- xs: bfloat16 [8192, 4096], P('seq', 'head'), may hold values from -6 to 6
- gate_branch: bfloat16 [8192, 4096], P('seq', 'head'), may hold values from -6 to 6
- bmat: bfloat16 [8192, 128], P('seq'), may hold values from -0.375 to 0.375
- cmat: bfloat16 [8192, 128], P('seq'), may hold values from -0.375 to 0.375
- dt_code: int32 [64, 8192], P('head', 'seq'), may hold values from 1 to 32768
- resets: int32 [8192], P('seq'), may hold values 0 or 1
- decay_rate: float32 [64], P('head'), may hold values from 4.8828125e-05 to 0.08, as said below
- skip: float32 [64], P('head'), may hold values from 0.5 to 1.5
- norm_gain: float32 [4096], P('head'), may hold values from 0.1 to 1.9
- out_weight: bfloat16 [4096, 4096], P('head'), may hold values from -0.09375 to 0.09375
Outputs:
- mixed: bfloat16 [8192, 4096], P(('seq', 'head'))
The draws below stay inside these ranges and needn't reach their ends.
Inputs may be any that keep to these rules, and one draw needn't show every extreme that they name: `decay_rate`: positive rates.
All inputs are finite; a program needn't handle non-finite values. No bound on the sum of `resets` on one device may be relied on, other than what follows from the above.
Results may differ from the reference program's by a relative error of at most 0.023.
Values may be sent and summed in bfloat16 or wider, within the bound.
A program may use at most 128 MiB of HBM per device.

```python
import jax
import jax.numpy as jnp
from jax import lax

D = 4096
HEADS = 64
HEAD_DIM = 64
STATE = 128
SPAN = 256
HORIZON_TICKS = 8192
INNER = 4096
GROUPS = 4


def draw_xs(key, part):
    first = jax.random.fold_in(key, 0)
    values = jax.random.normal(first, (HORIZON_TICKS, INNER), jnp.float32)
    return jnp.clip(values, -6.0, 6.0).astype(jnp.bfloat16)


def draw_dt_code(key, part):
    first, right_factor = jax.random.split(jax.random.fold_in(key, 11))
    starting_displacement = jax.random.randint(first, (HEADS, HORIZON_TICKS), 1, 17)
    contiguous_span_count = jax.random.randint(right_factor, (HORIZON_TICKS,), 0, HORIZON_TICKS) < 3
    return jnp.where(contiguous_span_count[None, :], 4 * HORIZON_TICKS, starting_displacement).astype(jnp.int32)


def draw_decay_rate(key, part):
    first, right_factor, third = jax.random.split(jax.random.fold_in(key, 23), 3)
    share = 0.5
    slow_mask = jax.random.uniform(first, (HEADS,), jnp.float32) < share
    slow_rate = jnp.exp(jax.random.uniform(right_factor, (HEADS,), jnp.float32, jnp.log(0.4), jnp.log(1.6))) / HORIZON_TICKS
    fast_rate = jnp.exp(jax.random.uniform(third, (HEADS,), jnp.float32, jnp.log(0.03), jnp.log(0.08)))
    return jnp.where(slow_mask, slow_rate, fast_rate).astype(jnp.float32)


def place_ends(drawn, key, low, high):
    longest = drawn.shape.index(max(drawn.shape))
    spots = []
    for shift in (0, 1):
        where = [jax.random.randint(jax.random.fold_in(key, axis), (), 0, length) for axis, length in enumerate(drawn.shape)]
        where[longest] = (where[longest] + shift) % drawn.shape[longest]
        spots.append(tuple(where))
    return drawn.at[spots[0]].set(low).at[spots[1]].set(high)


def shard_levels(rng, shape, shards, low, top_value):
    level, own = 1.0, jax.random.fold_in(rng, 6)
    for dim, parts in shards:
        draws = jnp.exp(jax.random.uniform(jax.random.fold_in(own, dim), (parts,), jnp.float32, low / len(shards), top_value / len(shards)))
        level = level * jnp.repeat(draws, shape[dim] // parts).reshape([-1 if axis == dim else 1 for axis in range(len(shape))])
    return level


def centred(own_key, shape, spread, reach, cuts=(), kind=jnp.bfloat16):
    entries = spread * jax.random.normal(own_key, shape, jnp.float32)
    if cuts:
        entries = entries * shard_levels(own_key, shape, cuts, -0.22, 0.18)
    return jnp.clip(entries, -reach, reach).astype(kind)


def setup_inputs(seed: int = 0) -> dict:
    key_of = jax.random.split(jax.random.key(seed), 11)
    xs = draw_xs(jax.random.fold_in(key_of[10], 71), 0)
    gate_branch = centred(key_of[1], (HORIZON_TICKS, INNER), 1.0, 6.0, ((0, 8), (1, 4)))
    bmat = centred(key_of[2], (HORIZON_TICKS, STATE), (2 * (HORIZON_TICKS * STATE) ** -0.25), 0.375, ((0, 8),))
    cmat = centred(key_of[3], (HORIZON_TICKS, STATE), (2 * (HORIZON_TICKS * STATE) ** -0.25), 0.375, ((0, 8),))
    dt_code = draw_dt_code(jax.random.fold_in(key_of[10], 71), 0)
    resets = place_ends((jax.random.randint(key_of[5], (HORIZON_TICKS,), 0, HORIZON_TICKS) < 2).astype(jnp.int32), jax.random.fold_in(key_of[5], 1), 0, 1)
    decay_rate = draw_decay_rate(jax.random.fold_in(key_of[10], 71), 0)
    skip = jnp.clip(0.5 + 1.0 * jax.random.uniform(key_of[7], (HEADS,), jnp.float32) ** shard_levels(key_of[7], (HEADS,), ((0, 4),), -0.2, 0.2), 0.5, 1.5)
    norm_gain = jnp.clip(1.0 + 0.18 * jax.random.normal(key_of[8], (INNER,), jnp.float32), 0.1, 1.9)
    out_weight = centred(key_of[9], (INNER, D), INNER ** -0.5, 0.09375, ((0, 4),))
    return {"xs": xs, "gate_branch": gate_branch, "bmat": bmat, "cmat": cmat, "dt_code": dt_code, "resets": resets, "decay_rate": decay_rate, "skip": skip, "norm_gain": norm_gain, "out_weight": out_weight}


def reference(xs, gate_branch, bmat, cmat, dt_code, resets, decay_rate, skip, norm_gain, out_weight):
    step_size = dt_code.astype(jnp.float32) / 16.0
    input_scale = jnp.minimum(step_size, 1.0)
    logarithmic_damping = -decay_rate[:, None] * step_size
    blocks = HORIZON_TICKS // SPAN
    values = xs.reshape(blocks, SPAN, HEADS, HEAD_DIM)
    key_blocks = bmat.reshape(blocks, SPAN, STATE)
    query_blocks = cmat.reshape(blocks, SPAN, STATE)
    log_blocks = logarithmic_damping.reshape(HEADS, blocks, SPAN).transpose(1, 0, 2)
    scale_blocks = input_scale.reshape(HEADS, blocks, SPAN).transpose(1, 0, 2)
    flag_blocks = resets.reshape(blocks, SPAN)

    def propagate_forward(state, inputs):
        value, key_rows, query, logs, scales, flags = inputs
        cumulative = jnp.cumsum(logs, axis=1)
        counts = jnp.cumsum(flags)
        position = jnp.arange(SPAN)
        linked = (counts[:, None] == counts[None, :]) & (position[None, :] <= position[:, None])
        gaps = jnp.where(linked[None], cumulative[:, :, None] - cumulative[:, None, :], 0.0)
        within = jnp.where(linked[None], jnp.exp(gaps), 0.0)
        intersection = jnp.dot(query, key_rows.T, preferred_element_type=jnp.float32)
        value_float = value.astype(jnp.float32)
        scaled = (value_float * scales.T[:, :, None]).astype(jnp.bfloat16)
        scaled_float = lax.optimization_barrier(scaled).astype(jnp.float32)
        scores = (within * intersection[None]).astype(jnp.bfloat16)
        scores_float = lax.optimization_barrier(scores).astype(jnp.float32)
        output = jnp.einsum('hij,jhp->ihp', scores_float, scaled_float, precision=lax.Precision.HIGHEST)
        from_start = jnp.where(counts[None, :] == 0, jnp.exp(cumulative), 0.0)
        query_float = query.astype(jnp.float32)
        carried = jnp.einsum('in,hpn->ihp', query_float, state, precision=lax.Precision.HIGHEST)
        output = output + carried * from_start.T[:, :, None]
        to_end = jnp.where(counts[None, :] == counts[-1], jnp.exp(cumulative[:, -1:] - cumulative), 0.0)
        through = jnp.where(counts[-1] == 0, jnp.exp(cumulative[:, -1]), 0.0)
        weighted = (scaled_float * to_end.T[:, :, None]).astype(jnp.bfloat16)
        weighted_float = lax.optimization_barrier(weighted).astype(jnp.float32)
        fresh = jnp.einsum('jhp,jn->hpn', weighted_float, key_rows.astype(jnp.float32), precision=lax.Precision.HIGHEST)
        state = through[:, None, None] * state + fresh
        output = output + skip[None, :, None] * value_float
        return (state, output)
    initial = jnp.zeros((HEADS, HEAD_DIM, STATE), jnp.float32)
    outputs = lax.scan(propagate_forward, initial, (values, key_blocks, query_blocks, log_blocks, scale_blocks, flag_blocks))[1]
    ssm_out = outputs.reshape(HORIZON_TICKS, INNER)
    gated = ssm_out * jax.nn.silu(gate_branch.astype(jnp.float32))
    mean_square = lax.optimization_barrier(jnp.mean(gated * gated, axis=1, keepdims=True))
    hidden = (gated * lax.rsqrt(mean_square + 1e-05) * norm_gain[None, :]).astype(jnp.bfloat16)
    group_width = INNER // GROUPS
    summed = jnp.zeros((HORIZON_TICKS, D), jnp.float32)
    for group in range(GROUPS):
        lower = group * group_width
        partial_value = jnp.dot(hidden[:, lower:lower + group_width], out_weight[lower:lower + group_width], preferred_element_type=jnp.float32).astype(jnp.bfloat16)
        summed = summed + lax.optimization_barrier(partial_value).astype(jnp.float32)
    return summed.astype(jnp.bfloat16)
```

```python
import functools

import jax
import jax.numpy as jnp
from jax import lax
from jax.experimental import pallas as pl
from jax.experimental.pallas import tpu as pltpu
from jax.sharding import PartitionSpec as P

HEAD_DIM = 64
SPAN = 256
QUARTERS = 4
F32 = jnp.float32
BF16 = jnp.bfloat16
MESH = pl.DeviceIdType.MESH
VMEM_BYTES = 60 * 1024 * 1024


def dot_nt(a, b):
    return lax.dot_general(a, b, (((1,), (1,)), ((), ())), preferred_element_type=F32)


def dot_tn(a, b):
    return lax.dot_general(a, b, (((0,), (0,)), ((), ())), preferred_element_type=F32)


def dot_nn(a, b):
    return jnp.dot(a, b, preferred_element_type=F32)


def two_pieces(v):
    high = v.astype(BF16)
    low = (v - high.astype(F32)).astype(BF16)
    return jnp.concatenate([high, low], axis=1)


def spread(heads):
    rows = lax.broadcasted_iota(jnp.int32, (2 * heads, heads * HEAD_DIM), 0)
    columns = lax.broadcasted_iota(jnp.int32, (2 * heads, heads * HEAD_DIM), 1)
    own = (columns // HEAD_DIM == rows) | (columns // HEAD_DIM == rows - heads)
    return jnp.where(own, 1.0, 0.0).astype(BF16)


def digits(code, flags):
    low = code & 127
    middle = (code >> 7) & 127
    high = code >> 14
    extra = jnp.broadcast_to(flags, code.shape)
    rows = jnp.concatenate([low, middle, high, extra], axis=0)
    return rows.astype(F32).astype(BF16)


def joined(sums, heads, axis):
    def take(n):
        return lax.slice_in_dim(sums, n * heads, (n + 1) * heads, axis=axis)

    return (take(0) + 128.0 * take(1) + 16384.0 * take(2)), take(3)


def final_kernel(x_ref, b_ref, code_ref, code_col_ref, flag_ref, rate_row_ref, rate_col_ref, out_ref):
    heads, ticks = code_ref.shape
    code = code_ref[...]
    parts = digits(code, flag_ref[...])
    i = lax.broadcasted_iota(jnp.int32, (ticks, ticks), 0)
    j = lax.broadcasted_iota(jnp.int32, (ticks, ticks), 1)
    later = jnp.where(j > i, 1.0, 0.0).astype(BF16)
    after, seen = joined(dot_nt(later, parts), heads, 1)
    scale = jnp.minimum(code_col_ref[...].astype(F32) / 16.0, 1.0)
    factor = jnp.where(seen == 0.0, jnp.exp(-rate_row_ref[...] * (after / 16.0)), 0.0) * scale
    wide = dot_nn(two_pieces(factor), spread(heads))
    weighted = (x_ref[...].astype(F32) * wide).astype(BF16)
    state = dot_tn(weighted, b_ref[...])
    rows = state.shape[0]
    out_ref[0:rows, :] = state.astype(BF16)
    every = jnp.ones((state.shape[1], ticks), BF16)
    total, resets = joined(dot_nt(parts, every), heads, 0)
    through = jnp.where(resets == 0.0, jnp.exp(-rate_col_ref[...] * (total / 16.0)), 0.0)
    high = through.astype(BF16)
    rest = through - high.astype(F32)
    middle = rest.astype(BF16)
    low = (rest - middle.astype(F32)).astype(BF16)
    lane = lax.broadcasted_iota(jnp.int32, through.shape, 1)
    packed = jnp.where(lane == 0, high.astype(F32), jnp.where(lane == 1, middle.astype(F32), low.astype(F32)))
    out_ref[rows : rows + heads, :] = packed.astype(BF16)


def intra_kernel(
    x_ref, b_ref, c_ref, code_ref, code_col_ref, flag_ref, rate_row_ref, rate_col_ref, skip_ref,
    ssm_ref, reach_ref, state, gone,
):
    heads = code_ref.shape[0]

    @pl.when(pl.program_id(0) == 0)
    def _():
        state[...] = jnp.zeros_like(state)
        gone[...] = jnp.zeros_like(gone)

    parts = digits(code_ref[...], flag_ref[...])
    i = lax.broadcasted_iota(jnp.int32, (SPAN, SPAN), 0)
    j = lax.broadcasted_iota(jnp.int32, (SPAN, SPAN), 1)
    upto = jnp.where(j <= i, 1.0, 0.0).astype(BF16)
    later = jnp.where(j > i, 1.0, 0.0).astype(BF16)
    sum_col, count_col = joined(dot_nt(upto, parts), heads, 1)
    after_col, seen_after = joined(dot_nt(later, parts), heads, 1)
    sum_row, count_row = joined(dot_nt(parts, upto), heads, 0)
    rate_row = rate_row_ref[...]
    cum_col = -rate_row * (sum_col / 16.0)
    cum_row = -rate_col_ref[...] * (sum_row / 16.0)
    eye = spread(heads)
    scale = jnp.minimum(code_col_ref[...].astype(F32) / 16.0, 1.0)
    to_end = jnp.where(seen_after == 0.0, jnp.exp(-rate_row * (after_col / 16.0)), 0.0)
    from_start = jnp.where(count_col == 0.0, jnp.exp(cum_col), 0.0)
    last = jnp.where(
        count_col[SPAN - 1 : SPAN] == 0.0, jnp.exp(cum_col[SPAN - 1 : SPAN]), 0.0
    )

    x = x_ref[...].astype(F32)
    wide_scale = dot_nn(scale.astype(BF16), eye[0:heads])
    scaled = (x * wide_scale).astype(BF16)
    b = b_ref[...]
    c = c_ref[...]
    linked = (count_col[:, 0:1] == count_row[0:1, :]) & (j <= i)
    cross = jnp.where(linked, dot_nt(c, b), 0.0)
    left = lax.broadcasted_iota(jnp.int32, (SPAN, 2 * HEAD_DIM), 1) < HEAD_DIM
    for pair in range(heads // 2):
        columns = slice(pair * 2 * HEAD_DIM, (pair + 1) * 2 * HEAD_DIM)
        both = scaled[:, columns]
        sides = []
        for h in (2 * pair, 2 * pair + 1):
            gap = jnp.minimum(cum_col[:, h : h + 1] - cum_row[h : h + 1, :], 0.0)
            scores = (jnp.exp(gap) * cross).astype(BF16)
            sides.append(dot_nn(scores, both))
        ssm_ref[:, columns] = jnp.where(left, sides[0], sides[1])
    old = state[...]
    carried = dot_nt(c, old.astype(BF16)) * dot_nn(two_pieces(from_start), eye)
    ssm_ref[...] = ssm_ref[...] + carried + skip_ref[...] * x
    weighted = (scaled.astype(F32) * dot_nn(two_pieces(to_end), eye)).astype(BF16)
    fresh = dot_tn(weighted, b)
    keep = dot_tn(eye, jnp.transpose(two_pieces(jnp.broadcast_to(last, (128, heads))).astype(F32)).astype(BF16))
    state[...] = keep * old + fresh
    before = gone[0:1, :]
    broken = gone[1:2, :]
    whole = jnp.where(
        (count_col + broken) == 0.0, jnp.exp(-rate_row * ((sum_col + before) / 16.0)), 0.0
    )
    reach_ref[...] = two_pieces(whole)
    gone[0:1, :] = before + sum_col[SPAN - 1 : SPAN]
    gone[1:2, :] = broken + count_col[SPAN - 1 : SPAN]


def mix_kernel(
    shards, seq_of, ssm_ref, gate_ref, c_ref, reach_ref, all_ref, gain_ref, w_hbm, out_ref,
    w, mine, incoming, kept, send1, recv1, send2, recv2, sq_send, sq_recv,
    w_sem, s1, r1, s2, r2, sqs, sqr,
):
    me = lax.axis_index("head")
    rank = lax.axis_index("seq")
    core = me % 2
    half = me // 2
    partner = half * 2 + (1 - core)
    across = (1 - half) * 2 + core
    diagonal = (1 - half) * 2 + (1 - core)
    inner = gate_ref.shape[1]
    width = out_ref.shape[1] // QUARTERS
    heads = inner // HEAD_DIM

    def load(q):
        return pltpu.make_async_copy(w_hbm.at[:, pl.ds(q * width, width)], w.at[q], w_sem.at[q])

    for q in range(QUARTERS):
        load(q).start()
    barrier = pltpu.get_barrier_semaphore()
    for other in (partner, across, diagonal):
        pl.semaphore_signal(barrier, inc=1, device_id={"head": other}, device_id_type=MESH)
    pl.semaphore_wait(barrier, 3)

    eye = spread(heads)
    incoming[...] = jnp.zeros_like(incoming)

    def take(n, _):
        pieces = all_ref[n, pl.ds(inner, heads), :].astype(F32)
        decay = pieces[:, 0:1] + pieces[:, 1:2] + pieces[:, 2:3]
        early = (n < rank).astype(F32)
        decay = early * decay + (1.0 - early)
        for h in range(heads):
            rows = slice(h * HEAD_DIM, (h + 1) * HEAD_DIM)
            fresh = all_ref[n, rows, :].astype(F32)
            incoming[rows, :] = decay[h : h + 1, :] * incoming[rows, :] + early * fresh
        return 0

    lax.fori_loop(0, shards, take, 0)
    start = incoming[...].astype(BF16)

    def prepare(block, slot):
        rows = pl.ds(pl.multiple_of(block * SPAN, SPAN), SPAN)
        carried = dot_nt(c_ref[rows, :], start) * dot_nn(reach_ref[rows, :], eye)
        gate = gate_ref[rows, :].astype(F32)
        gated = (ssm_ref[rows, :] + carried) * (gate / (1.0 + jnp.exp(-gate)))
        mine[...] = (gated * gain_ref[...]).astype(BF16)
        square = gated * gated
        high = square.astype(BF16)
        low = (square - high.astype(F32)).astype(BF16)
        ones = jnp.ones((8, inner), BF16)
        sq_send[slot] = dot_nt(ones, high) + dot_nt(ones, low)

    def square_copy(slot, other):
        return pltpu.make_async_remote_copy(
            src_ref=sq_send.at[slot], dst_ref=sq_recv.at[slot], send_sem=sqs.at[slot],
            recv_sem=sqr.at[slot], device_id={"head": other}, device_id_type=MESH,
        )

    def to_partner(turn, q):
        return pltpu.make_async_remote_copy(
            src_ref=send1.at[turn, q], dst_ref=recv1.at[turn, q], send_sem=s1.at[turn, q],
            recv_sem=r1.at[turn, q], device_id={"head": partner}, device_id_type=MESH,
        )

    def to_across(q):
        return pltpu.make_async_remote_copy(
            src_ref=send2.at[q], dst_ref=recv2.at[q], send_sem=s2.at[q],
            recv_sem=r2.at[q], device_id={"head": across}, device_id_type=MESH,
        )

    prepare(diagonal, 0)
    square_copy(0, diagonal).start()
    for q in range(QUARTERS):
        load(q).wait()

    def first(q, _):
        send1[0, q] = dot_nn(mine[...], w[q]).astype(BF16)
        to_partner(0, q).start()
        return 0

    lax.fori_loop(0, QUARTERS, first, 0)
    prepare(across, 1)
    square_copy(1, across).start()

    def second(q, _):
        part = dot_nn(mine[...], w[q])
        to_partner(0, q).wait_recv()
        send2[q] = (part + recv1[0, q].astype(F32)).astype(BF16)
        to_across(q).start()
        return 0

    lax.fori_loop(0, QUARTERS, second, 0)
    prepare(partner, 2)
    square_copy(2, partner).start()

    def third(q, _):
        send1[1, q] = dot_nn(mine[...], w[q]).astype(BF16)
        to_partner(1, q).start()
        return 0

    lax.fori_loop(0, QUARTERS, third, 0)
    prepare(me, 3)

    def fourth(q, _):
        part = dot_nn(mine[...], w[q])
        to_partner(1, q).wait_recv()
        kept[q] = part + recv1[1, q].astype(F32)
        return 0

    lax.fori_loop(0, QUARTERS, fourth, 0)
    for slot, other in enumerate((diagonal, across, partner)):
        square_copy(slot, other).wait()
    total = (sq_send[3] + sq_recv[0] + sq_recv[1] + sq_recv[2])[0:1, :]
    norm = lax.rsqrt(total / (4 * inner) + 1e-05)
    i = lax.broadcasted_iota(jnp.int32, (SPAN, SPAN), 0)
    j = lax.broadcasted_iota(jnp.int32, (SPAN, SPAN), 1)
    column = jnp.sum(jnp.where(i == j, norm, 0.0), axis=1, keepdims=True)
    for q in range(QUARTERS):
        to_across(q).wait_recv()
        out_ref[:, q * width : (q + 1) * width] = (
            (kept[q] + recv2[q].astype(F32)) * column
        ).astype(BF16)
    for q in range(QUARTERS):
        to_partner(0, q).wait_send()
        to_partner(1, q).wait_send()
        to_across(q).wait_send()


def local(shards, xs, gate_branch, bmat, cmat, dt_code, resets, decay_rate, skip, norm_gain, out_weight):
    ticks, inner = xs.shape
    heads = dt_code.shape[0]
    size = bmat.shape[1]
    model = out_weight.shape[1]
    code_col = dt_code.T
    flags = resets[None, :]
    rate_row = decay_rate[None, :]
    rate_col = decay_rate[:, None]
    wide_skip = jnp.repeat(skip, HEAD_DIM)[None, :]
    vmem = pl.BlockSpec(memory_space=pltpu.VMEM)
    final = pl.pallas_call(
        final_kernel,
        out_shape=jax.ShapeDtypeStruct((inner + heads, size), BF16),
        in_specs=[vmem] * 7,
        out_specs=vmem,
        compiler_params=pltpu.CompilerParams(vmem_limit_bytes=VMEM_BYTES),
        name="final_state",
    )(xs, bmat, dt_code, code_col, flags, rate_row, rate_col)
    gathered = lax.all_gather(final, "seq", axis=0, tiled=False)

    def whole(shape):
        return pl.BlockSpec(shape, lambda b: (0, 0))

    ssm, reach = pl.pallas_call(
        intra_kernel,
        grid=(ticks // SPAN,),
        out_shape=(
            jax.ShapeDtypeStruct((ticks, inner), F32),
            jax.ShapeDtypeStruct((ticks, 2 * heads), BF16),
        ),
        in_specs=[
            pl.BlockSpec((SPAN, inner), lambda b: (b, 0)),
            pl.BlockSpec((SPAN, size), lambda b: (b, 0)),
            pl.BlockSpec((SPAN, size), lambda b: (b, 0)),
            pl.BlockSpec((heads, SPAN), lambda b: (0, b)),
            pl.BlockSpec((SPAN, heads), lambda b: (b, 0)),
            pl.BlockSpec((1, SPAN), lambda b: (0, b)),
            whole((1, heads)),
            whole((heads, 1)),
            whole((1, inner)),
        ],
        out_specs=(
            pl.BlockSpec((SPAN, inner), lambda b: (b, 0)),
            pl.BlockSpec((SPAN, 2 * heads), lambda b: (b, 0)),
        ),
        scratch_shapes=[pltpu.VMEM((inner, size), F32), pltpu.VMEM((8, heads), F32)],
        compiler_params=pltpu.CompilerParams(vmem_limit_bytes=VMEM_BYTES // 2),
        cost_estimate=pl.CostEstimate(
            flops=12_000_000_000, bytes_accessed=8_000_000, transcendentals=5_000_000
        ),
        name="intra",
    )(xs, bmat, cmat, dt_code, code_col, flags, rate_row, rate_col, wide_skip)
    width = model // QUARTERS
    dma = pltpu.SemaphoreType.DMA
    return pl.pallas_call(
        functools.partial(mix_kernel, shards, None),
        out_shape=jax.ShapeDtypeStruct((SPAN, model), BF16),
        in_specs=[vmem] * 6 + [pl.BlockSpec(memory_space=pl.ANY)],
        out_specs=vmem,
        scratch_shapes=[
            pltpu.VMEM((QUARTERS, inner, width), BF16),
            pltpu.VMEM((SPAN, inner), BF16),
            pltpu.VMEM((inner, size), F32),
            pltpu.VMEM((QUARTERS, SPAN, width), F32),
            pltpu.VMEM((2, QUARTERS, SPAN, width), BF16),
            pltpu.VMEM((2, QUARTERS, SPAN, width), BF16),
            pltpu.VMEM((QUARTERS, SPAN, width), BF16),
            pltpu.VMEM((QUARTERS, SPAN, width), BF16),
            pltpu.VMEM((4, 8, SPAN), F32),
            pltpu.VMEM((3, 8, SPAN), F32),
            dma((QUARTERS,)),
            dma((2, QUARTERS)),
            dma((2, QUARTERS)),
            dma((QUARTERS,)),
            dma((QUARTERS,)),
            dma((3,)),
            dma((3,)),
        ],
        compiler_params=pltpu.CompilerParams(
            collective_id=0, has_side_effects=True, vmem_limit_bytes=VMEM_BYTES
        ),
        name="mix",
    )(ssm, gate_branch, cmat, reach, gathered, norm_gain[None, :], out_weight)


def solution(mesh):
    in_specs = (
        P("seq", "head"),
        P("seq", "head"),
        P("seq", None),
        P("seq", None),
        P("head", "seq"),
        P("seq"),
        P("head"),
        P("head"),
        P("head"),
        P("head", None),
    )
    out_specs = P(("seq", "head"), None)
    return jax.shard_map(
        functools.partial(local, mesh.shape["seq"]),
        mesh=mesh, in_specs=in_specs, out_specs=out_specs, check_vma=False,
    )
```

```python
import functools

import jax
import jax.numpy as jnp
from jax import lax
from jax.experimental import pallas as pl
from jax.experimental.pallas import tpu as pltpu
from jax.sharding import PartitionSpec as P

HEAD_DIM = 64
SPAN = 256
QUARTERS = 4
F32 = jnp.float32
BF16 = jnp.bfloat16
MESH = pl.DeviceIdType.MESH
VMEM_BYTES = 60 * 1024 * 1024


def dot_nt(a, b):
    return lax.dot_general(a, b, (((1,), (1,)), ((), ())), preferred_element_type=F32)


def dot_tn(a, b):
    return lax.dot_general(a, b, (((0,), (0,)), ((), ())), preferred_element_type=F32)


def dot_nn(a, b):
    return jnp.dot(a, b, preferred_element_type=F32)


def two_pieces(v):
    high = v.astype(BF16)
    low = (v - high.astype(F32)).astype(BF16)
    return jnp.concatenate([high, low], axis=1)


def spread(heads):
    rows = lax.broadcasted_iota(jnp.int32, (2 * heads, heads * HEAD_DIM), 0)
    columns = lax.broadcasted_iota(jnp.int32, (2 * heads, heads * HEAD_DIM), 1)
    own = (columns // HEAD_DIM == rows) | (columns // HEAD_DIM == rows - heads)
    return jnp.where(own, 1.0, 0.0).astype(BF16)


def digits(code, flags):
    low = code & 127
    middle = (code >> 7) & 127
    high = code >> 14
    extra = jnp.broadcast_to(flags, code.shape)
    rows = jnp.concatenate([low, middle, high, extra], axis=0)
    return rows.astype(F32).astype(BF16)


def joined(sums, heads, axis):
    def take(n):
        return lax.slice_in_dim(sums, n * heads, (n + 1) * heads, axis=axis)

    return (take(0) + 128.0 * take(1) + 16384.0 * take(2)), take(3)


def layer_kernel(
    shards, x_ref, gate_ref, b_ref, c_ref, code_ref, flag_ref, rate_ref, skip_ref, gain_ref, w_hbm, out_ref,
    w, ssm, reach, own, state, gone, final, other_final, decay, other_decay, came, passed, incoming,
    mine, kept, send1, recv1, send2, recv2, sq_send, sq_recv,
    w_sem, fs, fr, ds, dr, cs, cr, s1, r1, s2, r2, sqs, sqr,
):
    me = lax.axis_index("head")
    rank = lax.axis_index("seq")
    core = me % 2
    half = me // 2
    partner = half * 2 + (1 - core)
    across = (1 - half) * 2 + core
    diagonal = (1 - half) * 2 + (1 - core)
    odd = rank % 2
    twin = rank + 1 - 2 * odd
    ticks, inner = x_ref.shape
    heads = code_ref.shape[0]
    width = out_ref.shape[1] // QUARTERS
    blocks = ticks // SPAN
    pieces = heads // 2
    piece = inner // pieces

    def load(q):
        return pltpu.make_async_copy(w_hbm.at[:, pl.ds(q * width, width)], w.at[q], w_sem.at[q])

    for q in range(QUARTERS):
        load(q).start()

    @pl.when(rank < 2)
    def _():
        came[...] = jnp.zeros_like(came)

    barrier = pltpu.get_barrier_semaphore()
    for other in (partner, across, diagonal):
        pl.semaphore_signal(barrier, inc=1, device_id={"head": other}, device_id_type=MESH)
    for other in (twin, (rank + 2) % shards, (rank + shards - 2) % shards):
        pl.semaphore_signal(barrier, inc=1, device_id={"seq": other}, device_id_type=MESH)

    eye = spread(heads)
    rate_row = rate_ref[...]
    hi = lax.broadcasted_iota(jnp.int32, (heads, heads), 0)
    hj = lax.broadcasted_iota(jnp.int32, (heads, heads), 1)
    rate_col = jnp.sum(jnp.where(hi == hj, rate_row, 0.0), axis=1, keepdims=True)
    wide_skip = dot_nn(two_pieces(jnp.broadcast_to(skip_ref[...], (8, heads))), eye)[0:1]

    def scales(codes):
        return jnp.transpose(jnp.minimum(codes.astype(F32) / 16.0, 1.0))

    def local_final():
        parts = digits(code_ref[...], flag_ref[...])
        i = lax.broadcasted_iota(jnp.int32, (ticks, ticks), 0)
        j = lax.broadcasted_iota(jnp.int32, (ticks, ticks), 1)
        later = jnp.where(j > i, 1.0, 0.0).astype(BF16)
        after, seen = joined(dot_nt(later, parts), heads, 1)
        factor = jnp.where(seen == 0.0, jnp.exp(-rate_row * (after / 16.0)), 0.0)
        factor = factor * scales(code_ref[...])
        wide = dot_nn(two_pieces(factor), eye)
        weighted = (x_ref[...].astype(F32) * wide).astype(BF16)
        whole = dot_tn(weighted, b_ref[...])
        own[...] = whole
        final[...] = whole.astype(BF16)
        every = jnp.ones((whole.shape[1], ticks), BF16)
        total, resets = joined(dot_nt(parts, every), heads, 0)
        decay[...] = jnp.where(resets == 0.0, jnp.exp(-rate_col * (total / 16.0)), 0.0)

    def final_copy(q):
        rows = pl.ds(q * piece, piece)
        return pltpu.make_async_remote_copy(
            src_ref=final.at[rows], dst_ref=other_final.at[rows], send_sem=fs.at[q],
            recv_sem=fr.at[q], device_id={"seq": twin}, device_id_type=MESH,
        )

    def decay_copy():
        return pltpu.make_async_remote_copy(
            src_ref=decay, dst_ref=other_decay, send_sem=ds.at[0],
            recv_sem=dr.at[0], device_id={"seq": twin}, device_id_type=MESH,
        )

    def chain_copy(q):
        rows = pl.ds(q * piece, piece)
        return pltpu.make_async_remote_copy(
            src_ref=passed.at[rows], dst_ref=came.at[rows], send_sem=cs.at[q],
            recv_sem=cr.at[q], device_id={"seq": (rank + 2) % shards}, device_id_type=MESH,
        )

    local_final()
    pl.semaphore_wait(barrier, 6)
    decay_copy().start()
    for q in range(pieces):
        final_copy(q).start()

    state[...] = jnp.zeros_like(state)
    gone[...] = jnp.zeros_like(gone)

    def intra(block, _):
        start = pl.multiple_of(block * SPAN, SPAN)
        rows = pl.ds(start, SPAN)
        codes = code_ref[:, rows]
        parts = digits(codes, flag_ref[:, rows])
        i = lax.broadcasted_iota(jnp.int32, (SPAN, SPAN), 0)
        j = lax.broadcasted_iota(jnp.int32, (SPAN, SPAN), 1)
        upto = jnp.where(j <= i, 1.0, 0.0).astype(BF16)
        later = jnp.where(j > i, 1.0, 0.0).astype(BF16)
        sum_col, count_col = joined(dot_nt(upto, parts), heads, 1)
        after_col, seen_after = joined(dot_nt(later, parts), heads, 1)
        sum_row, count_row = joined(dot_nt(parts, upto), heads, 0)
        cum_col = -rate_row * (sum_col / 16.0)
        cum_row = -rate_col * (sum_row / 16.0)
        to_end = jnp.where(seen_after == 0.0, jnp.exp(-rate_row * (after_col / 16.0)), 0.0)
        from_start = jnp.where(count_col == 0.0, jnp.exp(cum_col), 0.0)
        last = jnp.where(
            count_col[SPAN - 1 : SPAN] == 0.0, jnp.exp(cum_col[SPAN - 1 : SPAN]), 0.0
        )
        x = x_ref[rows, :].astype(F32)
        scaled = (x * dot_nn(scales(codes).astype(BF16), eye[0:heads])).astype(BF16)
        b = b_ref[rows, :]
        c = c_ref[rows, :]
        linked = (count_col[:, 0:1] == count_row[0:1, :]) & (j <= i)
        cross = jnp.where(linked, dot_nt(c, b), 0.0)
        left = lax.broadcasted_iota(jnp.int32, (SPAN, 2 * HEAD_DIM), 1) < HEAD_DIM
        old = state[...]
        carried = dot_nt(c, old.astype(BF16)) * dot_nn(two_pieces(from_start), eye)
        carried = carried + wide_skip * x
        for pair in range(heads // 2):
            columns = slice(pair * 2 * HEAD_DIM, (pair + 1) * 2 * HEAD_DIM)
            both = scaled[:, columns]
            sides = []
            for h in (2 * pair, 2 * pair + 1):
                gap = jnp.minimum(cum_col[:, h : h + 1] - cum_row[h : h + 1, :], 0.0)
                scores = (jnp.exp(gap) * cross).astype(BF16)
                sides.append(dot_nn(scores, both))
            ssm[rows, columns] = jnp.where(left, sides[0], sides[1]) + carried[:, columns]
        weighted = (scaled.astype(F32) * dot_nn(two_pieces(to_end), eye)).astype(BF16)
        fresh = dot_tn(weighted, b)
        spread_last = two_pieces(jnp.broadcast_to(last, (128, heads))).astype(F32)
        state[...] = dot_tn(eye, jnp.transpose(spread_last).astype(BF16)) * old + fresh
        before = gone[0:1, :]
        broken = gone[1:2, :]
        whole = jnp.where(
            (count_col + broken) == 0.0, jnp.exp(-rate_row * ((sum_col + before) / 16.0)), 0.0
        )
        reach[rows, :] = two_pieces(whole)
        gone[0:1, :] = before + sum_col[SPAN - 1 : SPAN]
        gone[1:2, :] = broken + count_col[SPAN - 1 : SPAN]
        return 0

    lax.fori_loop(0, blocks - 1, intra, 0)

    decay_copy().wait_recv()
    odd_f = odd.astype(F32)
    even_f = 1.0 - odd_f
    ours = decay[...]
    theirs = other_decay[...]
    second_decay = odd_f * ours + even_f * theirs
    both_decay = ours * theirs
    step_decay = odd_f * theirs + even_f
    for q in range(pieces):
        final_copy(q).wait_recv()

        @pl.when(rank >= 2)
        def _():
            chain_copy(q).wait_recv()

        for h in range(2 * q, 2 * q + 2):
            rows = slice(h * HEAD_DIM, (h + 1) * HEAD_DIM)
            here = own[rows, :]
            there = other_final[rows, :].astype(F32)
            before = came[rows, :].astype(F32)
            first = odd_f * there + even_f * here
            second = odd_f * here + even_f * there
            total = second_decay[h : h + 1, :] * first + second
            passed[rows, :] = (both_decay[h : h + 1, :] * before + total).astype(BF16)
            incoming[rows, :] = (step_decay[h : h + 1, :] * before + odd_f * there).astype(BF16)

        @pl.when(rank < shards - 2)
        def _():
            chain_copy(q).start()

    lax.fori_loop(blocks - 1, blocks, intra, 0)
    start = incoming[...]

    def prepare(block, slot):
        rows = pl.ds(pl.multiple_of(block * SPAN, SPAN), SPAN)
        carried = dot_nt(c_ref[rows, :], start) * dot_nn(reach[rows, :], eye)
        gate = gate_ref[rows, :].astype(F32)
        gated = (ssm[rows, :] + carried) * (gate / (1.0 + jnp.exp(-gate)))
        mine[...] = (gated * gain_ref[...]).astype(BF16)
        square = gated * gated
        high = square.astype(BF16)
        low = (square - high.astype(F32)).astype(BF16)
        ones = jnp.ones((8, inner), BF16)
        sq_send[slot] = dot_nt(ones, high) + dot_nt(ones, low)

    def square_copy(slot, other):
        return pltpu.make_async_remote_copy(
            src_ref=sq_send.at[slot], dst_ref=sq_recv.at[slot], send_sem=sqs.at[slot],
            recv_sem=sqr.at[slot], device_id={"head": other}, device_id_type=MESH,
        )

    def to_partner(turn, q):
        return pltpu.make_async_remote_copy(
            src_ref=send1.at[turn, q], dst_ref=recv1.at[turn, q], send_sem=s1.at[turn, q],
            recv_sem=r1.at[turn, q], device_id={"head": partner}, device_id_type=MESH,
        )

    def to_across(q):
        return pltpu.make_async_remote_copy(
            src_ref=send2.at[q], dst_ref=recv2.at[q], send_sem=s2.at[q],
            recv_sem=r2.at[q], device_id={"head": across}, device_id_type=MESH,
        )

    prepare(diagonal, 0)
    square_copy(0, diagonal).start()
    for q in range(QUARTERS):
        load(q).wait()

    def first(q, _):
        send1[0, q] = dot_nn(mine[...], w[q]).astype(BF16)
        to_partner(0, q).start()
        return 0

    lax.fori_loop(0, QUARTERS, first, 0)
    prepare(across, 1)
    square_copy(1, across).start()

    def second(q, _):
        part = dot_nn(mine[...], w[q])
        to_partner(0, q).wait_recv()
        send2[q] = (part + recv1[0, q].astype(F32)).astype(BF16)
        to_across(q).start()
        return 0

    lax.fori_loop(0, QUARTERS, second, 0)
    prepare(partner, 2)
    square_copy(2, partner).start()

    def third(q, _):
        send1[1, q] = dot_nn(mine[...], w[q]).astype(BF16)
        to_partner(1, q).start()
        return 0

    lax.fori_loop(0, QUARTERS, third, 0)
    prepare(me, 3)

    def fourth(q, _):
        part = dot_nn(mine[...], w[q])
        to_partner(1, q).wait_recv()
        kept[q] = part + recv1[1, q].astype(F32)
        return 0

    lax.fori_loop(0, QUARTERS, fourth, 0)
    for slot, other in enumerate((diagonal, across, partner)):
        square_copy(slot, other).wait()
    total = (sq_send[3] + sq_recv[0] + sq_recv[1] + sq_recv[2])[0:1, :]
    norm = lax.rsqrt(total / (4 * inner) + 1e-05)
    i = lax.broadcasted_iota(jnp.int32, (SPAN, SPAN), 0)
    j = lax.broadcasted_iota(jnp.int32, (SPAN, SPAN), 1)
    column = jnp.sum(jnp.where(i == j, norm, 0.0), axis=1, keepdims=True)
    for q in range(QUARTERS):
        to_across(q).wait_recv()
        out_ref[:, q * width : (q + 1) * width] = (
            (kept[q] + recv2[q].astype(F32)) * column
        ).astype(BF16)
    for q in range(QUARTERS):
        to_partner(0, q).wait_send()
        to_partner(1, q).wait_send()
        to_across(q).wait_send()
    for q in range(pieces):
        final_copy(q).wait_send()
    decay_copy().wait_send()

    @pl.when(rank < shards - 2)
    def _():
        for q in range(pieces):
            chain_copy(q).wait_send()


def local(shards, xs, gate_branch, bmat, cmat, dt_code, resets, decay_rate, skip, norm_gain, out_weight):
    ticks, inner = xs.shape
    heads = dt_code.shape[0]
    size = bmat.shape[1]
    model = out_weight.shape[1]
    width = model // QUARTERS
    pieces = heads // 2
    vmem = pl.BlockSpec(memory_space=pltpu.VMEM)
    dma = pltpu.SemaphoreType.DMA
    return pl.pallas_call(
        functools.partial(layer_kernel, shards),
        out_shape=jax.ShapeDtypeStruct((SPAN, model), BF16),
        in_specs=[vmem] * 9 + [pl.BlockSpec(memory_space=pl.ANY)],
        out_specs=vmem,
        scratch_shapes=[
            pltpu.VMEM((QUARTERS, inner, width), BF16),
            pltpu.VMEM((ticks, inner), F32),
            pltpu.VMEM((ticks, 2 * heads), BF16),
            pltpu.VMEM((inner, size), F32),
            pltpu.VMEM((inner, size), F32),
            pltpu.VMEM((8, heads), F32),
            pltpu.VMEM((inner, size), BF16),
            pltpu.VMEM((inner, size), BF16),
            pltpu.VMEM((heads, size), F32),
            pltpu.VMEM((heads, size), F32),
            pltpu.VMEM((inner, size), BF16),
            pltpu.VMEM((inner, size), BF16),
            pltpu.VMEM((inner, size), BF16),
            pltpu.VMEM((SPAN, inner), BF16),
            pltpu.VMEM((QUARTERS, SPAN, width), F32),
            pltpu.VMEM((2, QUARTERS, SPAN, width), BF16),
            pltpu.VMEM((2, QUARTERS, SPAN, width), BF16),
            pltpu.VMEM((QUARTERS, SPAN, width), BF16),
            pltpu.VMEM((QUARTERS, SPAN, width), BF16),
            pltpu.VMEM((4, 8, SPAN), F32),
            pltpu.VMEM((3, 8, SPAN), F32),
            dma((QUARTERS,)),
            dma((pieces,)),
            dma((pieces,)),
            dma((1,)),
            dma((1,)),
            dma((pieces,)),
            dma((pieces,)),
            dma((2, QUARTERS)),
            dma((2, QUARTERS)),
            dma((QUARTERS,)),
            dma((QUARTERS,)),
            dma((3,)),
            dma((3,)),
        ],
        compiler_params=pltpu.CompilerParams(
            collective_id=0, has_side_effects=True, vmem_limit_bytes=VMEM_BYTES
        ),
        name="layer",
    )(
        xs, gate_branch, bmat, cmat, dt_code, resets[None, :], decay_rate[None, :], skip[None, :],
        norm_gain[None, :], out_weight,
    )


def solution(mesh):
    in_specs = (
        P("seq", "head"),
        P("seq", "head"),
        P("seq", None),
        P("seq", None),
        P("head", "seq"),
        P("seq"),
        P("head"),
        P("head"),
        P("head"),
        P("head", None),
    )
    out_specs = P(("seq", "head"), None)
    return jax.shard_map(
        functools.partial(local, mesh.shape["seq"]),
        mesh=mesh, in_specs=in_specs, out_specs=out_specs, check_vma=False,
    )
```
